32 devices in a mesh: pole: 4 (over x, core), row: 4 (over z), col: 2 (over y).
Axes of the slice: x: 2, y: 2, z: 4, core: 2. Of those that a mesh axis runs over, the one named last changes fastest.
Arguments:
- anc_inverse: bfloat16 [4, 2, 4, 192, 768], P('pole', None, None, 'col', 'row'), may hold values from -6 to 6
- panel: bfloat16 [4, 2, 768, 1024], P('pole', None, ('row', 'col')), may hold values from -0.21875 to 0.21875
- pattern: int32 [8, 2], replicated, may hold values 0 or 1
- diag_inverse: bfloat16 [4, 2, 1024, 512], P('pole', None, 'col', 'row'), may hold values from -6 to 6
- pole_weights: float32 [4, 2], P('pole'), may hold values from -4 to 4
Outputs:
- inv_panel: float32 [4, 2, 768, 1024], P('pole', None, 'row', 'col')
- inv_diag: bfloat16 [4, 2, 1024, 512], P('pole', None, 'col', 'row')
- density: float32 [1024, 512], P('col', 'row')
The draws below stay inside these ranges and needn't reach their ends.
All inputs are finite; a program needn't handle non-finite values.
Results may differ from the reference program's by a relative error of at most 0.013.
Values may be sent and summed in bfloat16 or wider, within the bound.
A program may use at most 128 MiB of HBM per device.

```python
import jax
import jax.numpy as jnp
from jax import lax

W = 512
ANC_DEV = 96
POLES = 4
NK = 2
KW = 1024
NFB = 8
NA = 768
NQ = 4


def plant(values, rng, smallest, high):
    place = [jax.random.randint(jax.random.fold_in(rng, axis), (), 0, length) for axis, length in enumerate(values.shape)]
    main_axis = values.shape.index(max(values.shape))
    next_to = place[:main_axis] + [(place[main_axis] + 1) % values.shape[main_axis]] + place[main_axis + 1:]
    return values.at[tuple(place)].set(smallest).at[tuple(next_to)].set(high)


def block_scale(key, dims, pieces, smallest, top_value):
    factor_of = 1.0
    for axis_at, blocks in pieces:
        steps = jax.random.uniform(jax.random.fold_in(jax.random.fold_in(key, 6), axis_at), (blocks,), jnp.float32, smallest / len(pieces), top_value / len(pieces))
        factor_of = factor_of * jnp.repeat(jnp.exp(steps), dims[axis_at] // blocks).reshape((-1,) + (1,) * (len(dims) - 1 - axis_at))
    return factor_of


def bell_draw(own_key, dims, spread, most, split=(), held_as=jnp.bfloat16):
    loudness = block_scale(own_key, dims, split, -0.22, 0.18) if split else 1.0
    values = jax.random.normal(own_key, dims, jnp.float32) * spread * loudness
    return jnp.minimum(jnp.maximum(values, -most), most).astype(held_as)


def setup_inputs(seed: int = 0) -> dict:
    splits = jax.random.split(jax.random.key(seed), 6)
    return {
        "anc_inverse": bell_draw(splits[0], (POLES, 2, NQ, NA // NQ, NA), 1.0, 6.0, ((0, 4), (3, 2), (4, 4))),
        "panel": bell_draw(splits[1], (POLES, 2, NA, KW), NA ** -0.5, 0.21875, ((0, 4), (2, 8))),
        "pattern": plant((jax.random.randint(splits[2], (NFB, NK), 0, 3) < 2).astype(jnp.int32), jax.random.fold_in(splits[2], 1), 0, 1),
        "diag_inverse": bell_draw(splits[3], (POLES, 2, KW, W), 1.0, 6.0, ((0, 4), (2, 2), (3, 4))),
        "pole_weights": bell_draw(splits[4], (POLES, 2), 1.0, 4.0, ((0, 4),), jnp.float32),
    }


def complex_product(left_re, left_im, right_re, right_im):
    exact = lax.Precision.HIGHEST
    left_re = left_re.astype(jnp.float32)
    left_im = left_im.astype(jnp.float32)
    right_re = right_re.astype(jnp.float32)
    right_im = right_im.astype(jnp.float32)
    real_part = jnp.dot(left_re.T, right_re, precision=exact) - jnp.dot(left_im.T, right_im, precision=exact)
    imag_part = jnp.dot(left_im.T, right_re, precision=exact) + jnp.dot(left_re.T, right_im, precision=exact)
    return real_part, imag_part


def reference(anc_inverse, panel, pattern, diag_inverse, pole_weights):
    exact = lax.Precision.HIGHEST
    keep_mask = jnp.repeat(jnp.repeat(pattern.astype(jnp.bfloat16), W, axis=1), ANC_DEV, axis=0)

    def contract(first, second):
        return jnp.einsum('jka,jkb->kab', first, second, precision=exact)

    def one_pole(inputs):
        ancestor, factor, diagonal = inputs
        transposed = ancestor.reshape(2, NA, NA)
        masked = factor * keep_mask[None]
        prod_re, prod_im = complex_product(transposed[0], transposed[1], masked[0], masked[1])
        result_panel = jnp.stack([-prod_re, -prod_im])
        rounded = lax.optimization_barrier(result_panel.astype(jnp.bfloat16)).astype(jnp.float32)
        factor_full = masked.astype(jnp.float32).reshape(2, NA, NK, W)
        panel_full = rounded.reshape(2, NA, NK, W)
        diag_re = contract(factor_full[0], panel_full[0]) - contract(factor_full[1], panel_full[1])
        diag_im = contract(factor_full[0], panel_full[1]) + contract(factor_full[1], panel_full[0])
        result_diag = diagonal.astype(jnp.float32) - jnp.stack([diag_re, diag_im]).reshape(2, KW, W)
        return result_panel, result_diag

    inv_panel, diag_full = lax.map(one_pole, (anc_inverse, panel, diag_inverse))
    density = jnp.einsum('p,pab->ab', pole_weights[:, 0], diag_full[:, 1], precision=exact)
    density = density + jnp.einsum('p,pab->ab', pole_weights[:, 1], diag_full[:, 0], precision=exact)
    return inv_panel, diag_full.astype(jnp.bfloat16), density
```

```python
import functools

import jax
import jax.numpy as jnp
from jax import lax
from jax.experimental import pallas as pl
from jax.experimental.pallas import tpu as pltpu
from jax.sharding import PartitionSpec as P

MESH = pl.DeviceIdType.MESH
F32 = jnp.float32
BF16 = jnp.bfloat16


def tdot(a, b):
    return lax.dot_general(a, b, (((0,), (0,)), ((), ())), preferred_element_type=F32)


def kernel(
    n_pole, n_row, n_col,
    anc, panel, pattern, diag_in, weight,
    inv_out, diag_out, dens,
    g, p, pm, acc, r_send, r_relay, r_full, s1_send, s1_recv, s2_send, s2_recv,
    loc_sem, ys, yr, gs, gr, zs, zr, fs, fr, rs, rr, ps, pr,
):
    me_p = lax.axis_index("pole")
    me_r = lax.axis_index("row")
    me_c = lax.axis_index("col")
    right = lax.rem(me_r + 1, n_row)
    left = lax.rem(me_r + n_row - 1, n_row)
    opp = lax.rem(me_r + 2, n_row)
    core = lax.rem(me_p, 2)
    partner = me_p + 1 - 2 * core
    n_x = n_pole // 2
    block = panel.shape[2]
    width = p.shape[2] // 2
    n_i = anc.shape[4]
    cols = r_send.shape[2] // 2

    def remote(src, dst, send, recv, **where):
        return pltpu.make_async_remote_copy(
            src_ref=src, dst_ref=dst, send_sem=send, recv_sem=recv, device_id=where, device_id_type=MESH)

    def hrows(h):
        return pl.ds(pl.multiple_of(h * block, 16), block)

    def pcols(o):
        return pl.ds(pl.multiple_of(o * width, 128), width)

    local = []
    for t in range(2):
        cp = pltpu.make_async_copy(
            panel.at[0, t, :, pcols(me_c)], p.at[me_r, hrows(me_c), pl.ds(t * width, width)], loc_sem.at[t])
        cp.start()
        local.append(cp)

    x_of = [lax.rem(me_p + 2 * j, n_pole) for j in range(1, n_x)]
    c_of = [lax.rem(me_c + j, n_col) for j in range(1, n_col)]
    barrier = pltpu.get_barrier_semaphore()
    peers = [{"row": right}, {"row": left}, {"pole": partner}]
    peers += [{"col": o} for o in c_of] + [{"pole": o} for o in x_of]
    for where in peers:
        pl.semaphore_signal(barrier, inc=1, device_id=where, device_id_type=MESH)

    for q in range(n_row):
        g[q, me_c] = jnp.concatenate([anc[0, 0, q], anc[0, 1, q]], axis=1)

    for cp in local:
        cp.wait()
    pl.semaphore_wait(barrier, len(peers))

    h_of = [lax.rem(me_c + n_col - k, n_col) for k in range(n_col)]
    y_copies, g_copies = {}, {}
    for j in range(1, n_col):
        for t in range(2):
            y_copies[j, t] = remote(
                panel.at[0, t, :, pcols(c_of[j - 1])], p.at[me_r, hrows(me_c), pl.ds(t * width, width)],
                ys.at[j - 1, t], yr.at[j - 1, t], col=c_of[j - 1])

    def z_pair(k):
        piece = p.at[me_r, hrows(h_of[k])]
        return (remote(piece, piece, zs.at[0, k], zr.at[0, k], row=right),
                remote(piece, piece, zs.at[1, k], zr.at[1, k], row=left))

    def f_pair(k):
        a = p.at[left, hrows(h_of[k]), pl.ds(0, width)]
        b = p.at[right, hrows(h_of[k]), pl.ds(width, width)]
        return (remote(a, a, fs.at[0, k], fr.at[0, k], row=right),
                remote(b, b, fs.at[1, k], fr.at[1, k], row=left))

    z_copies = [z_pair(k) for k in range(n_col)]
    f_copies = [f_pair(k) for k in range(n_col)]
    for k in range(n_col):
        for j in range(1, n_col):
            if k == 0:
                for t in range(2):
                    y_copies[j, t].start()
        if k > 0:
            y_copies[k, 0].wait_recv()
            y_copies[k, 1].wait_recv()
        for cp in z_copies[k]:
            cp.start()
    for j in range(1, n_col):
        g_copies[j] = remote(g.at[:, me_c], g.at[:, me_c], gs.at[j - 1], gr.at[j - 1], col=c_of[j - 1])
        g_copies[j].start()

    def mask_block(q):
        for h in range(n_col):
            keep = pattern[q * n_col + h, me_c].astype(F32)
            rows = pl.ds(h * block, block)
            pm[q, rows, :] = p[q, rows, :] * jnp.full((1, 2 * width), keep, F32).astype(BF16)

    m_all = 2 * n_i
    m_tile = m_all if m_all <= 512 else 384
    n_tile = 512

    def product(q, first):
        def tile(m0, n0):
            a = g[q, :, :, pl.ds(m0, m_tile)].reshape(n_col * block, m_tile)
            b = pm[q, :, pl.ds(n0, n_tile)]
            v = tdot(a, b)
            where = (pl.ds(m0, m_tile), pl.ds(n0, n_tile))
            acc[where] = v if first else acc[where] + v

        if m_all == m_tile:
            for n in range(2 * width // n_tile):
                tile(0, n * n_tile)
        else:
            @pl.loop(0, m_all // m_tile)
            def _(m):
                for n in range(2 * width // n_tile):
                    tile(pl.multiple_of(m * m_tile, 128), n * n_tile)

    mask_block(me_r)
    for k in range(n_col):
        z_copies[k][0].wait_recv()
        f_copies[k][0].start()
        z_copies[k][1].wait_recv()
        f_copies[k][1].start()
    mask_block(left)
    mask_block(right)
    for j in range(1, n_col):
        g_copies[j].wait_recv()
    product(me_r, True)
    product(left, False)
    product(right, False)
    for k in range(n_col):
        for cp in f_copies[k]:
            cp.wait_recv()
    mask_block(opp)
    product(opp, False)

    for s in range(n_row):
        re_cols = pl.ds(s * cols, cols)
        im_cols = pl.ds(width + s * cols, cols)
        re = acc[pl.ds(n_i, n_i), im_cols] - acc[pl.ds(0, n_i), re_cols]
        im = -(acc[pl.ds(n_i, n_i), re_cols] + acc[pl.ds(0, n_i), im_cols])
        inv_out[0, 0, :, re_cols] = re
        inv_out[0, 1, :, re_cols] = im
        r_send[s] = jnp.concatenate([re.astype(BF16), im.astype(BF16)], axis=1)
    r_full[me_r] = r_send[me_r]

    lo, hi = pl.ds(0, cols), pl.ds(cols, cols)
    first_leg = [
        remote(r_send.at[opp, :, lo], r_relay.at[0], rs.at[0], rr.at[0], row=right),
        remote(r_send.at[opp, :, hi], r_relay.at[1], rs.at[1], rr.at[1], row=left),
    ]
    direct = [
        remote(r_send.at[right], r_full.at[me_r], rs.at[2], rr.at[2], row=right),
        remote(r_send.at[left], r_full.at[me_r], rs.at[3], rr.at[3], row=left),
    ]
    second_leg = [
        remote(r_relay.at[0], r_full.at[left, :, lo], rs.at[4], rr.at[4], row=right),
        remote(r_relay.at[1], r_full.at[right, :, hi], rs.at[5], rr.at[5], row=left),
    ]
    for cp in first_leg + direct:
        cp.start()
    for a, b in zip(first_leg, second_leg):
        a.wait_recv()
        b.start()
    for cp in direct + second_leg:
        cp.wait_recv()

    half = width // 2
    w_re = weight[0, 0]
    w_im = weight[0, 1]

    def density_half(start):
        re = jnp.zeros((half, cols), F32)
        im = jnp.zeros((half, cols), F32)
        for q in range(n_row):
            r = r_full[q]
            a = tdot(pm[q, :, pl.ds(start, half)], r)
            b = tdot(pm[q, :, pl.ds(pl.multiple_of(width + start, 128), half)], r)
            re = re + a[:, :cols] - b[:, cols:]
            im = im + a[:, cols:] + b[:, :cols]
        rows = pl.ds(start, half)
        re = diag_in[0, 0, rows, :].astype(F32) - re
        im = diag_in[0, 1, rows, :].astype(F32) - im
        diag_out[0, 0, rows, :] = re.astype(BF16)
        diag_out[0, 1, rows, :] = im.astype(BF16)
        return w_re * im + w_im * re

    mine = pl.multiple_of(core * half, half)
    other = pl.multiple_of((1 - core) * half, half)
    s1_send[...] = density_half(other)
    swap = remote(s1_send, s1_recv, ps.at[0], pr.at[0], pole=partner)
    swap.start()
    own = density_half(mine)
    swap.wait_recv()
    s2_send[...] = (own + s1_recv[...]).astype(BF16)
    across = []
    for j in range(1, n_x):
        cp = remote(s2_send, s2_recv.at[j - 1], ps.at[1 + j], pr.at[1 + j], pole=x_of[j - 1])
        cp.start()
        across.append(cp)
    total = s2_send[...].astype(F32)
    for j in range(1, n_x):
        across[j - 1].wait_recv()
        total = total + s2_recv[j - 1].astype(F32)
    dens[pl.ds(mine, half), :] = total
    piece = dens.at[pl.ds(mine, half)]
    back = remote(piece, piece, ps.at[1], pr.at[1], pole=partner)
    back.start()
    back.wait_recv()

    sent = list(y_copies.values()) + list(g_copies.values())
    sent += [cp for pair in z_copies + f_copies for cp in pair]
    sent += first_leg + direct + second_leg + [swap, back] + across
    for cp in sent:
        cp.wait_send()


def body(n_pole, n_row, n_col, anc, panel, pattern, diag_in, weight):
    block = panel.shape[2]
    width = panel.shape[3] // n_col
    n_i = anc.shape[4]
    cols = diag_in.shape[3]
    n_x = n_pole // 2
    dma = pltpu.SemaphoreType.DMA
    vmem = pl.BlockSpec(memory_space=pltpu.VMEM)
    smem = pl.BlockSpec(memory_space=pltpu.SMEM)
    return pl.pallas_call(
        functools.partial(kernel, n_pole, n_row, n_col),
        out_shape=(
            jax.ShapeDtypeStruct((1, 2, n_i, width), F32),
            jax.ShapeDtypeStruct((1, 2, width, cols), BF16),
            jax.ShapeDtypeStruct((width, cols), F32),
        ),
        in_specs=[vmem, vmem, smem, vmem, smem],
        out_specs=(vmem, vmem, vmem),
        scratch_shapes=[
            pltpu.VMEM((n_row, n_col, block, 2 * n_i), BF16),
            pltpu.VMEM((n_row, n_col * block, 2 * width), BF16),
            pltpu.VMEM((n_row, n_col * block, 2 * width), BF16),
            pltpu.VMEM((2 * n_i, 2 * width), F32),
            pltpu.VMEM((n_row, n_i, 2 * cols), BF16),
            pltpu.VMEM((2, n_i, cols), BF16),
            pltpu.VMEM((n_row, n_i, 2 * cols), BF16),
            pltpu.VMEM((width // 2, cols), F32),
            pltpu.VMEM((width // 2, cols), F32),
            pltpu.VMEM((width // 2, cols), BF16),
            pltpu.VMEM((max(n_x - 1, 1), width // 2, cols), BF16),
            dma((2,)),
            dma((n_col - 1, 2)), dma((n_col - 1, 2)),
            dma((n_col - 1,)), dma((n_col - 1,)),
            dma((2, n_col)), dma((2, n_col)),
            dma((2, n_col)), dma((2, n_col)),
            dma((6,)), dma((6,)),
            dma((n_x + 1,)), dma((n_x + 1,)),
        ],
        compiler_params=pltpu.CompilerParams(
            collective_id=0, has_side_effects=True, vmem_limit_bytes=60 * 1024 * 1024),
        name="selinv",
    )(anc, panel, pattern, diag_in, weight)


def solution(mesh):
    shape = mesh.shape
    placed = (
        P("pole", None, None, "col", "row"),
        P("pole", None, ("row", "col"), None),
        P(),
        P("pole", None, "col", "row"),
        P("pole", None),
    )
    return jax.shard_map(
        functools.partial(body, shape["pole"], shape["row"], shape["col"]),
        mesh=mesh,
        in_specs=placed,
        out_specs=(P("pole", None, "row", "col"), P("pole", None, "col", "row"), P("col", "row")),
        check_vma=False,
    )
```

```python
import functools

import jax
import jax.numpy as jnp
from jax import lax
from jax.experimental import pallas as pl
from jax.experimental.pallas import tpu as pltpu
from jax.sharding import PartitionSpec as P

MESH = pl.DeviceIdType.MESH
F32 = jnp.float32
BF16 = jnp.bfloat16


def tdot(a, b):
    return lax.dot_general(a, b, (((0,), (0,)), ((), ())), preferred_element_type=F32)


def kernel(
    n_pole, n_row, n_col,
    anc, panel, pattern, diag_in, weight,
    inv_out, diag_out, dens,
    g, p, pm, acc, r_send, r_full, s1_send, s1_recv, s2_send, s2_recv,
    loc_sem, ys, yr, gs, gr, zs, zr, rs, rr, ps, pr,
):
    me_p = lax.axis_index("pole")
    me_r = lax.axis_index("row")
    me_c = lax.axis_index("col")
    right = lax.rem(me_r + 1, n_row)
    left = lax.rem(me_r + n_row - 1, n_row)
    core = lax.rem(me_p, 2)
    partner = me_p + 1 - 2 * core
    n_x = n_pole // 2
    block = panel.shape[2]
    width = p.shape[2] // 2
    n_i = anc.shape[4]
    cols = r_send.shape[2] // 2

    def remote(src, dst, send, recv, **where):
        return pltpu.make_async_remote_copy(
            src_ref=src, dst_ref=dst, send_sem=send, recv_sem=recv, device_id=where, device_id_type=MESH)

    def hrows(h):
        return pl.ds(pl.multiple_of(h * block, 16), block)

    def pcols(o):
        return pl.ds(pl.multiple_of(o * width, 128), width)

    local = []
    for t in range(2):
        cp = pltpu.make_async_copy(
            panel.at[0, t, :, pcols(me_c)], p.at[me_r, hrows(me_c), pl.ds(t * width, width)], loc_sem.at[t])
        cp.start()
        local.append(cp)

    x_of = [lax.rem(me_p + 2 * j, n_pole) for j in range(1, n_x)]
    c_of = [lax.rem(me_c + j, n_col) for j in range(1, n_col)]
    barrier = pltpu.get_barrier_semaphore()
    r_of = [lax.rem(me_r + j, n_row) for j in range(1, n_row)]
    peers = [{"pole": partner}] + [{"row": o} for o in r_of]
    peers += [{"col": o} for o in c_of] + [{"pole": o} for o in x_of]
    for where in peers:
        pl.semaphore_signal(barrier, inc=1, device_id=where, device_id_type=MESH)

    for q in range(n_row):
        g[q, me_c] = jnp.concatenate([anc[0, 0, q], anc[0, 1, q]], axis=1)

    for cp in local:
        cp.wait()
    pl.semaphore_wait(barrier, len(peers))

    h_of = [lax.rem(me_c + n_col - k, n_col) for k in range(n_col)]
    y_copies, g_copies = {}, {}
    for j in range(1, n_col):
        for t in range(2):
            y_copies[j, t] = remote(
                panel.at[0, t, :, pcols(c_of[j - 1])], p.at[me_r, hrows(me_c), pl.ds(t * width, width)],
                ys.at[j - 1, t], yr.at[j - 1, t], col=c_of[j - 1])

    last = n_row - 1

    def moving_right(d, k):
        piece = p.at[lax.rem(me_r + n_row - (d - 1), n_row), hrows(h_of[k])]
        return remote(piece, piece, zs.at[0, d - 1, k], zr.at[0, d - 1, k], row=right)

    def moving_left(d, k):
        piece = p.at[lax.rem(me_r + d - 1, n_row), hrows(h_of[k])]
        return remote(piece, piece, zs.at[1, d - 1, k], zr.at[1, d - 1, k], row=left)

    def from_left(d, k):
        piece = p.at[lax.rem(me_r + n_row - d, n_row), hrows(h_of[k])]
        return remote(piece, piece, zs.at[0, d - 1, k], zr.at[0, d - 1, k], row=right)

    def from_right(d, k):
        piece = p.at[lax.rem(me_r + d, n_row), hrows(h_of[k])]
        return remote(piece, piece, zs.at[1, d - 1, k], zr.at[1, d - 1, k], row=left)

    for k in range(n_col):
        if k == 0:
            for cp in y_copies.values():
                cp.start()
        else:
            y_copies[k, 0].wait_recv()
            y_copies[k, 1].wait_recv()

        @pl.when(me_r < last)
        def _():
            moving_right(1, k).start()

        @pl.when(me_r > 0)
        def _():
            moving_left(1, k).start()

    for j in range(1, n_col):
        g_copies[j] = remote(g.at[:, me_c], g.at[:, me_c], gs.at[j - 1], gr.at[j - 1], col=c_of[j - 1])
        g_copies[j].start()

    def mask_block(q):
        for h in range(n_col):
            row = pattern[pl.ds(q * n_col + h, 1), :].astype(F32)
            lane = lax.broadcasted_iota(jnp.int32, row.shape, 1)
            keep = jnp.sum(jnp.where(lane == me_c, row, 0.0), axis=1, keepdims=True)
            rows = pl.ds(h * block, block)
            pm[q, rows, :] = p[q, rows, :] * jnp.broadcast_to(keep, (1, 2 * width)).astype(BF16)

    m_all = 2 * n_i
    m_tile = m_all if m_all <= 512 else 384
    n_tile = 512

    def product(q, first):
        def tile(m0, n0):
            a = g[q, :, :, pl.ds(m0, m_tile)].reshape(n_col * block, m_tile)
            b = pm[q, :, pl.ds(n0, n_tile)]
            v = tdot(a, b)
            where = (pl.ds(m0, m_tile), pl.ds(n0, n_tile))
            acc[where] = v if first else acc[where] + v

        if m_all == m_tile:
            for n in range(2 * width // n_tile):
                tile(0, n * n_tile)
        else:
            @pl.loop(0, m_all // m_tile)
            def _(m):
                for n in range(2 * width // n_tile):
                    tile(pl.multiple_of(m * m_tile, 128), n * n_tile)

    mask_block(me_r)
    for d in range(1, n_row):
        for k in range(n_col):
            @pl.when(me_r >= d)
            def _():
                from_left(d, k).wait_recv()

                @pl.when(me_r < last)
                def _():
                    moving_right(d + 1, k).start()

            @pl.when(me_r <= last - d)
            def _():
                from_right(d, k).wait_recv()

                @pl.when(me_r > 0)
                def _():
                    moving_left(d + 1, k).start()

        if d == 1:
            for cp in g_copies.values():
                cp.wait_recv()
            product(me_r, True)

        @pl.when(me_r >= d)
        def _():
            q = lax.rem(me_r + n_row - d, n_row)
            mask_block(q)
            product(q, False)

        @pl.when(me_r <= last - d)
        def _():
            q = lax.rem(me_r + d, n_row)
            mask_block(q)
            product(q, False)

    for s in range(n_row):
        re_cols = pl.ds(s * cols, cols)
        im_cols = pl.ds(width + s * cols, cols)
        re = acc[pl.ds(n_i, n_i), im_cols] - acc[pl.ds(0, n_i), re_cols]
        im = -(acc[pl.ds(n_i, n_i), re_cols] + acc[pl.ds(0, n_i), im_cols])
        inv_out[0, 0, :, re_cols] = re.astype(BF16)
        inv_out[0, 1, :, re_cols] = im.astype(BF16)
        r_send[s] = jnp.concatenate([re.astype(BF16), im.astype(BF16)], axis=1)
    r_full[me_r] = r_send[me_r]

    order = [2, 3, 1] if n_row == 4 else list(range(1, n_row))
    direct = [
        remote(r_send.at[r_of[j - 1]], r_full.at[me_r], rs.at[j - 1], rr.at[j - 1], row=r_of[j - 1])
        for j in order
    ]
    for cp in direct:
        cp.start()
    for cp in direct:
        cp.wait_recv()

    half = width // 2
    w_re = weight[0, 0]
    w_im = weight[0, 1]

    def density_half(start):
        re = jnp.zeros((half, cols), F32)
        im = jnp.zeros((half, cols), F32)
        for q in range(n_row):
            r = r_full[q]
            a = tdot(pm[q, :, pl.ds(start, half)], r)
            b = tdot(pm[q, :, pl.ds(pl.multiple_of(width + start, 128), half)], r)
            re = re + a[:, :cols] - b[:, cols:]
            im = im + a[:, cols:] + b[:, :cols]
        rows = pl.ds(start, half)
        re = diag_in[0, 0, rows, :].astype(F32) - re
        im = diag_in[0, 1, rows, :].astype(F32) - im
        diag_out[0, 0, rows, :] = re.astype(BF16)
        diag_out[0, 1, rows, :] = im.astype(BF16)
        return w_re * im + w_im * re

    mine = pl.multiple_of(core * half, half)
    other = pl.multiple_of((1 - core) * half, half)
    s1_send[...] = density_half(other)
    swap = remote(s1_send, s1_recv, ps.at[0], pr.at[0], pole=partner)
    swap.start()
    own = density_half(mine)
    swap.wait_recv()
    s2_send[...] = (own + s1_recv[...]).astype(BF16)
    across = []
    for j in range(1, n_x):
        cp = remote(s2_send, s2_recv.at[j - 1], ps.at[1 + j], pr.at[1 + j], pole=x_of[j - 1])
        cp.start()
        across.append(cp)
    total = s2_send[...].astype(F32)
    for j in range(1, n_x):
        across[j - 1].wait_recv()
        total = total + s2_recv[j - 1].astype(F32)
    dens[pl.ds(mine, half), :] = total
    piece = dens.at[pl.ds(mine, half)]
    back = remote(piece, piece, ps.at[1], pr.at[1], pole=partner)
    back.start()
    back.wait_recv()

    sent = list(y_copies.values()) + list(g_copies.values())
    sent += direct + [swap, back] + across
    for cp in sent:
        cp.wait_send()
    for d in range(1, n_row):
        for k in range(n_col):
            @pl.when((me_r < last) & (me_r >= d - 1))
            def _():
                moving_right(d, k).wait_send()

            @pl.when((me_r > 0) & (me_r <= last - (d - 1)))
            def _():
                moving_left(d, k).wait_send()


def body(n_pole, n_row, n_col, anc, panel, pattern, diag_in, weight):
    block = panel.shape[2]
    width = panel.shape[3] // n_col
    n_i = anc.shape[4]
    cols = diag_in.shape[3]
    n_x = n_pole // 2
    dma = pltpu.SemaphoreType.DMA
    vmem = pl.BlockSpec(memory_space=pltpu.VMEM)
    smem = pl.BlockSpec(memory_space=pltpu.SMEM)
    inv, diag, dens = pl.pallas_call(
        functools.partial(kernel, n_pole, n_row, n_col),
        out_shape=(
            jax.ShapeDtypeStruct((1, 2, n_i, width), BF16),
            jax.ShapeDtypeStruct((1, 2, width, cols), BF16),
            jax.ShapeDtypeStruct((width, cols), F32),
        ),
        in_specs=[vmem, vmem, vmem, vmem, smem],
        out_specs=(vmem, vmem, vmem),
        scratch_shapes=[
            pltpu.VMEM((n_row, n_col, block, 2 * n_i), BF16),
            pltpu.VMEM((n_row, n_col * block, 2 * width), BF16),
            pltpu.VMEM((n_row, n_col * block, 2 * width), BF16),
            pltpu.VMEM((2 * n_i, 2 * width), F32),
            pltpu.VMEM((n_row, n_i, 2 * cols), BF16),
            pltpu.VMEM((n_row, n_i, 2 * cols), BF16),
            pltpu.VMEM((width // 2, cols), F32),
            pltpu.VMEM((width // 2, cols), F32),
            pltpu.VMEM((width // 2, cols), BF16),
            pltpu.VMEM((max(n_x - 1, 1), width // 2, cols), BF16),
            dma((2,)),
            dma((n_col - 1, 2)), dma((n_col - 1, 2)),
            dma((n_col - 1,)), dma((n_col - 1,)),
            dma((2, n_row - 1, n_col)), dma((2, n_row - 1, n_col)),
            dma((n_row - 1,)), dma((n_row - 1,)),
            dma((n_x + 1,)), dma((n_x + 1,)),
        ],
        compiler_params=pltpu.CompilerParams(
            collective_id=0, has_side_effects=True, vmem_limit_bytes=60 * 1024 * 1024),
        name="selinv",
    )(anc, panel, pattern, diag_in, weight)
    return inv.astype(F32), diag, dens


def solution(mesh):
    shape = mesh.shape
    placed = (
        P("pole", None, None, "col", "row"),
        P("pole", None, ("row", "col"), None),
        P(),
        P("pole", None, "col", "row"),
        P("pole", None),
    )
    return jax.shard_map(
        functools.partial(body, shape["pole"], shape["row"], shape["col"]),
        mesh=mesh,
        in_specs=placed,
        out_specs=(P("pole", None, "row", "col"), P("pole", None, "col", "row"), P("col", "row")),
        check_vma=False,
    )
```

```python
import functools

import jax
import jax.numpy as jnp
from jax import lax
from jax.experimental import pallas as pl
from jax.experimental.pallas import tpu as pltpu
from jax.sharding import PartitionSpec as P

MESH = pl.DeviceIdType.MESH
F32 = jnp.float32
BF16 = jnp.bfloat16


def tdot(a, b):
    return lax.dot_general(a, b, (((0,), (0,)), ((), ())), preferred_element_type=F32)


def kernel(
    n_pole, n_row, n_col,
    anc, panel, pattern, diag_in, weight,
    inv_out, diag_out, dens,
    g, p, pm, acc, r_send, r_full, s1_send, s1_recv, s2_send, s2_recv,
    loc_sem, ys, yr, gs, gr, zs, zr, rs, rr, ps, pr,
):
    me_p = lax.axis_index("pole")
    me_r = lax.axis_index("row")
    me_c = lax.axis_index("col")
    right = lax.rem(me_r + 1, n_row)
    left = lax.rem(me_r + n_row - 1, n_row)
    core = lax.rem(me_p, 2)
    partner = me_p + 1 - 2 * core
    n_x = n_pole // 2
    block = panel.shape[2]
    width = p.shape[2] // 2
    n_i = anc.shape[4]
    cols = r_send.shape[2] // 2

    def remote(src, dst, send, recv, **where):
        return pltpu.make_async_remote_copy(
            src_ref=src, dst_ref=dst, send_sem=send, recv_sem=recv, device_id=where, device_id_type=MESH)

    def hrows(h):
        return pl.ds(pl.multiple_of(h * block, 16), block)

    def pcols(o):
        return pl.ds(pl.multiple_of(o * width, 128), width)

    local = []
    for t in range(2):
        cp = pltpu.make_async_copy(
            panel.at[0, t, :, pcols(me_c)], p.at[me_r, hrows(me_c), pl.ds(t * width, width)], loc_sem.at[t])
        cp.start()
        local.append(cp)

    x_of = [lax.rem(me_p + 2 * j, n_pole) for j in range(1, n_x)]
    c_of = [lax.rem(me_c + j, n_col) for j in range(1, n_col)]
    barrier = pltpu.get_barrier_semaphore()
    r_of = [lax.rem(me_r + j, n_row) for j in range(1, n_row)]
    peers = [{"pole": partner}] + [{"row": o} for o in r_of]
    peers += [{"col": o} for o in c_of] + [{"pole": o} for o in x_of]
    for where in peers:
        pl.semaphore_signal(barrier, inc=1, device_id=where, device_id_type=MESH)

    for q in range(n_row):
        g[q, me_c] = jnp.concatenate([anc[0, 0, q], anc[0, 1, q]], axis=1)

    for cp in local:
        cp.wait()
    pl.semaphore_wait(barrier, len(peers))

    h_of = [lax.rem(me_c + n_col - k, n_col) for k in range(n_col)]
    y_copies, g_copies = {}, {}
    for j in range(1, n_col):
        for t in range(2):
            y_copies[j, t] = remote(
                panel.at[0, t, :, pcols(c_of[j - 1])], p.at[me_r, hrows(me_c), pl.ds(t * width, width)],
                ys.at[j - 1, t], yr.at[j - 1, t], col=c_of[j - 1])

    last = n_row - 1

    def moving_right(d, k):
        piece = p.at[lax.rem(me_r + n_row - (d - 1), n_row), hrows(h_of[k // 2]), pl.ds(k % 2 * width, width)]
        return remote(piece, piece, zs.at[0, d - 1, k], zr.at[0, d - 1, k], row=right)

    def moving_left(d, k):
        piece = p.at[lax.rem(me_r + d - 1, n_row), hrows(h_of[k // 2]), pl.ds(k % 2 * width, width)]
        return remote(piece, piece, zs.at[1, d - 1, k], zr.at[1, d - 1, k], row=left)

    def from_left(d, k):
        piece = p.at[lax.rem(me_r + n_row - d, n_row), hrows(h_of[k // 2]), pl.ds(k % 2 * width, width)]
        return remote(piece, piece, zs.at[0, d - 1, k], zr.at[0, d - 1, k], row=right)

    def from_right(d, k):
        piece = p.at[lax.rem(me_r + d, n_row), hrows(h_of[k // 2]), pl.ds(k % 2 * width, width)]
        return remote(piece, piece, zs.at[1, d - 1, k], zr.at[1, d - 1, k], row=left)

    for k in range(2 * n_col):
        if k == 0:
            for cp in y_copies.values():
                cp.start()
        if k >= 2:
            y_copies[k // 2, k % 2].wait_recv()

        @pl.when(me_r < last)
        def _():
            moving_right(1, k).start()

        @pl.when(me_r > 0)
        def _():
            moving_left(1, k).start()

    for j in range(1, n_col):
        g_copies[j] = remote(g.at[:, me_c], g.at[:, me_c], gs.at[j - 1], gr.at[j - 1], col=c_of[j - 1])
        g_copies[j].start()

    def mask_block(q):
        for h in range(n_col):
            row = pattern[pl.ds(q * n_col + h, 1), :].astype(F32)
            lane = lax.broadcasted_iota(jnp.int32, row.shape, 1)
            keep = jnp.sum(jnp.where(lane == me_c, row, 0.0), axis=1, keepdims=True)
            rows = pl.ds(h * block, block)
            pm[q, rows, :] = p[q, rows, :] * jnp.broadcast_to(keep, (1, 2 * width)).astype(BF16)

    m_all = 2 * n_i
    m_tile = m_all if m_all <= 512 else 384
    n_tile = 512

    def product(q, first):
        def tile(m0, n0):
            a = g[q, :, :, pl.ds(m0, m_tile)].reshape(n_col * block, m_tile)
            b = pm[q, :, pl.ds(n0, n_tile)]
            v = tdot(a, b)
            where = (pl.ds(m0, m_tile), pl.ds(n0, n_tile))
            acc[where] = v if first else acc[where] + v

        if m_all == m_tile:
            for n in range(2 * width // n_tile):
                tile(0, n * n_tile)
        else:
            @pl.loop(0, m_all // m_tile)
            def _(m):
                for n in range(2 * width // n_tile):
                    tile(pl.multiple_of(m * m_tile, 128), n * n_tile)

    mask_block(me_r)
    for d in range(1, n_row):
        for k in range(2 * n_col):
            @pl.when(me_r >= d)
            def _():
                from_left(d, k).wait_recv()

                @pl.when(me_r < last)
                def _():
                    moving_right(d + 1, k).start()

            @pl.when(me_r <= last - d)
            def _():
                from_right(d, k).wait_recv()

                @pl.when(me_r > 0)
                def _():
                    moving_left(d + 1, k).start()

        if d == 1:
            for cp in g_copies.values():
                cp.wait_recv()
            product(me_r, True)

        @pl.when(me_r >= d)
        def _():
            q = lax.rem(me_r + n_row - d, n_row)
            mask_block(q)
            product(q, False)

        @pl.when(me_r <= last - d)
        def _():
            q = lax.rem(me_r + d, n_row)
            mask_block(q)
            product(q, False)

    for s in range(n_row):
        re_cols = pl.ds(s * cols, cols)
        im_cols = pl.ds(width + s * cols, cols)
        re = acc[pl.ds(n_i, n_i), im_cols] - acc[pl.ds(0, n_i), re_cols]
        im = -(acc[pl.ds(n_i, n_i), re_cols] + acc[pl.ds(0, n_i), im_cols])
        inv_out[0, 0, :, re_cols] = re.astype(BF16)
        inv_out[0, 1, :, re_cols] = im.astype(BF16)
        r_send[s] = jnp.concatenate([re.astype(BF16), im.astype(BF16)], axis=1)
    r_full[me_r] = r_send[me_r]

    order = [2, 3, 1] if n_row == 4 else list(range(1, n_row))
    direct = [
        remote(r_send.at[r_of[j - 1]], r_full.at[me_r], rs.at[j - 1], rr.at[j - 1], row=r_of[j - 1])
        for j in order
    ]
    for cp in direct:
        cp.start()
    for cp in direct:
        cp.wait_recv()

    half = width // 2
    w_re = weight[0, 0]
    w_im = weight[0, 1]

    def density_half(start):
        re = jnp.zeros((half, cols), F32)
        im = jnp.zeros((half, cols), F32)
        for q in range(n_row):
            r = r_full[q]
            a = tdot(pm[q, :, pl.ds(start, half)], r)
            b = tdot(pm[q, :, pl.ds(pl.multiple_of(width + start, 128), half)], r)
            re = re + a[:, :cols] - b[:, cols:]
            im = im + a[:, cols:] + b[:, :cols]
        rows = pl.ds(start, half)
        re = diag_in[0, 0, rows, :].astype(F32) - re
        im = diag_in[0, 1, rows, :].astype(F32) - im
        diag_out[0, 0, rows, :] = re.astype(BF16)
        diag_out[0, 1, rows, :] = im.astype(BF16)
        return w_re * im + w_im * re

    mine = pl.multiple_of(core * half, half)
    other = pl.multiple_of((1 - core) * half, half)
    s1_send[...] = density_half(other)
    swap = remote(s1_send, s1_recv, ps.at[0], pr.at[0], pole=partner)
    swap.start()
    own = density_half(mine)
    swap.wait_recv()
    s2_send[...] = (own + s1_recv[...]).astype(BF16)
    across = []
    for j in range(1, n_x):
        cp = remote(s2_send, s2_recv.at[j - 1], ps.at[1 + j], pr.at[1 + j], pole=x_of[j - 1])
        cp.start()
        across.append(cp)
    total = s2_send[...].astype(F32)
    for j in range(1, n_x):
        across[j - 1].wait_recv()
        total = total + s2_recv[j - 1].astype(F32)
    dens[pl.ds(mine, half), :] = total
    piece = dens.at[pl.ds(mine, half)]
    back = remote(piece, piece, ps.at[1], pr.at[1], pole=partner)
    back.start()
    back.wait_recv()

    sent = list(y_copies.values()) + list(g_copies.values())
    sent += direct + [swap, back] + across
    for cp in sent:
        cp.wait_send()
    for d in range(1, n_row):
        for k in range(2 * n_col):
            @pl.when((me_r < last) & (me_r >= d - 1))
            def _():
                moving_right(d, k).wait_send()

            @pl.when((me_r > 0) & (me_r <= last - (d - 1)))
            def _():
                moving_left(d, k).wait_send()


def body(n_pole, n_row, n_col, anc, panel, pattern, diag_in, weight):
    block = panel.shape[2]
    width = panel.shape[3] // n_col
    n_i = anc.shape[4]
    cols = diag_in.shape[3]
    n_x = n_pole // 2
    dma = pltpu.SemaphoreType.DMA
    vmem = pl.BlockSpec(memory_space=pltpu.VMEM)
    smem = pl.BlockSpec(memory_space=pltpu.SMEM)
    inv, diag, dens = pl.pallas_call(
        functools.partial(kernel, n_pole, n_row, n_col),
        out_shape=(
            jax.ShapeDtypeStruct((1, 2, n_i, width), BF16),
            jax.ShapeDtypeStruct((1, 2, width, cols), BF16),
            jax.ShapeDtypeStruct((width, cols), F32),
        ),
        in_specs=[vmem, vmem, vmem, vmem, smem],
        out_specs=(vmem, vmem, vmem),
        scratch_shapes=[
            pltpu.VMEM((n_row, n_col, block, 2 * n_i), BF16),
            pltpu.VMEM((n_row, n_col * block, 2 * width), BF16),
            pltpu.VMEM((n_row, n_col * block, 2 * width), BF16),
            pltpu.VMEM((2 * n_i, 2 * width), F32),
            pltpu.VMEM((n_row, n_i, 2 * cols), BF16),
            pltpu.VMEM((n_row, n_i, 2 * cols), BF16),
            pltpu.VMEM((width // 2, cols), F32),
            pltpu.VMEM((width // 2, cols), F32),
            pltpu.VMEM((width // 2, cols), BF16),
            pltpu.VMEM((max(n_x - 1, 1), width // 2, cols), BF16),
            dma((2,)),
            dma((n_col - 1, 2)), dma((n_col - 1, 2)),
            dma((n_col - 1,)), dma((n_col - 1,)),
            dma((2, n_row - 1, 2 * n_col)), dma((2, n_row - 1, 2 * n_col)),
            dma((n_row - 1,)), dma((n_row - 1,)),
            dma((n_x + 1,)), dma((n_x + 1,)),
        ],
        compiler_params=pltpu.CompilerParams(
            collective_id=0, has_side_effects=True, vmem_limit_bytes=60 * 1024 * 1024),
        name="selinv",
    )(anc, panel, pattern, diag_in, weight)
    return inv.astype(F32), diag, dens


def solution(mesh):
    shape = mesh.shape
    placed = (
        P("pole", None, None, "col", "row"),
        P("pole", None, ("row", "col"), None),
        P(),
        P("pole", None, "col", "row"),
        P("pole", None),
    )
    return jax.shard_map(
        functools.partial(body, shape["pole"], shape["row"], shape["col"]),
        mesh=mesh,
        in_specs=placed,
        out_specs=(P("pole", None, "row", "col"), P("pole", None, "col", "row"), P("col", "row")),
        check_vma=False,
    )
```
